32 devices in a mesh: grp: 4 (over y, core), blk: 8 (over z, x).
Axes of the slice: x: 2, y: 2, z: 4, core: 2. Of those that a mesh axis runs over, the one named last changes fastest.
Arguments:
- queries: bfloat16 [4, 128, 4096], P(None, ('blk', 'grp')), may hold values from -24 to 24
- cache_keys: bfloat16 [4, 3584, 512], P('grp', 'blk'), may hold values from -24 to 24
- cache_values: bfloat16 [4, 3584, 512], P('grp', 'blk'), may hold values from -15 to 15
- new_keys: bfloat16 [4, 128, 512], P(None, ('blk', 'grp')), may hold values from -6 to 6
- new_values: bfloat16 [4, 128, 512], P(None, ('blk', 'grp')), may hold values from -15 to 15
- hits: int32 [4], P('grp'), may hold values from 448 to 3584, as said below
- counts: int32 [4], P('grp'), may hold values from 64 to 128, as said below
- assign: int32 [4, 8], P('grp'), may hold values from 0 to 7, each once within a row
Outputs:
- attended: bfloat16 [4, 128, 4096], P(None, ('blk', 'grp'))
The draws below stay inside these ranges and needn't reach their ends.
Inputs may be any that keep to these rules, and one draw needn't show every extreme that they name: Cached positions of request r below hits[r] are valid; in every draw some request has all 3584 valid. New tokens of request r at order counts[r] or later are padding; in every draw some request has all 128.
All inputs are finite; a program needn't handle non-finite values.
Results may differ from the reference program's by a relative error of at most 0.0085.
Values may be sent and summed in bfloat16 or wider, within the bound.
A program may use at most 128 MiB of HBM per device.

```python
import jax
import jax.numpy as jnp
from jax import lax

HEADS = 32
KV_HEADS = 4
HEAD_DIM = 128
Q_DEV = 16
C_DEV = 448
REQ = 4
NEW = 128
CTX = 3584
N_BLK = 8


def shared_keys(key):
    return jnp.clip(jax.random.normal(jax.random.fold_in(key, 11), (REQ, CTX, KV_HEADS * HEAD_DIM), jnp.float32), -5.0, 5.0)


def draw_cache_keys(key, part):
    keys = shared_keys(key)
    return keys.astype(jnp.bfloat16)


def draw_queries(key, part):
    base = 2.0 * jnp.clip(jax.random.normal(jax.random.fold_in(key, 12), (REQ, NEW, HEADS * HEAD_DIM), jnp.float32), -5.0, 5.0)
    return base.astype(jnp.bfloat16)


def draw_hits(key, part):
    values = jax.random.randint(jax.random.fold_in(key, 21), (REQ,), CTX // 8, CTX + 1, jnp.int32)
    chosen = jax.random.randint(jax.random.fold_in(key, 22), (), 0, REQ, jnp.int32)
    return values.at[chosen].set(CTX)


def draw_counts(key, part):
    values = jax.random.randint(jax.random.fold_in(key, 31), (REQ,), NEW // 2, NEW + 1, jnp.int32)
    chosen = jax.random.randint(jax.random.fold_in(key, 32), (), 0, REQ, jnp.int32)
    return values.at[chosen].set(NEW)


def level_of(own_key, dims, pieces, low, largest):
    def one(dim, blocks):
        heights = jax.random.uniform(jax.random.fold_in(jax.random.fold_in(own_key, 6), dim), (blocks,), jnp.float32, low / len(pieces), largest / len(pieces))
        return jnp.repeat(jnp.exp(heights), dims[dim] // blocks).reshape((-1,) + (1,) * (len(dims) - dim - 1))

    gain = one(*pieces[0])
    for cut in pieces[1:]:
        gain = gain * one(*cut)
    return gain


def normal_values(key, extent, scale, most, cuts=(), kind=jnp.bfloat16):
    array = jax.random.normal(key, extent, jnp.float32) * scale
    if len(cuts) > 0:
        array = level_of(key, extent, cuts, -0.22, 0.18) * array
    return jnp.clip(array, min=-most, max=most).astype(kind)


def setup_inputs(seed: int = 0) -> dict:
    key_of = jax.random.split(jax.random.key(seed), 9)
    return {
        "queries": draw_queries(jax.random.fold_in(key_of[8], 71), 0),
        "cache_keys": draw_cache_keys(jax.random.fold_in(key_of[8], 71), 0),
        "cache_values": normal_values(key_of[2], (REQ, CTX, KV_HEADS * HEAD_DIM), 3.0, 15.0, ((0, 4), (1, 8))),
        "new_keys": normal_values(key_of[3], (REQ, NEW, KV_HEADS * HEAD_DIM), 1.0, 6.0, ((1, 32),)),
        "new_values": normal_values(key_of[4], (REQ, NEW, KV_HEADS * HEAD_DIM), 3.0, 15.0, ((1, 32),)),
        "hits": draw_hits(jax.random.fold_in(key_of[8], 71), 0),
        "counts": draw_counts(jax.random.fold_in(key_of[8], 71), 0),
        "assign": jax.vmap(lambda own: jax.random.permutation(own, N_BLK))(jax.random.split(key_of[7], REQ)).reshape((REQ, N_BLK)).astype(jnp.int32),
    }


def partial_block(queries, keys, values, allowed, kv_heads):
    row_count, full_width = queries.shape
    key_count = keys.shape[0]
    head_dim = keys.shape[1] // kv_heads
    group_size = full_width // head_dim // kv_heads
    query_heads = queries.astype(jnp.float32).reshape(row_count, kv_heads, group_size, head_dim)
    key_heads = keys.astype(jnp.float32).reshape(key_count, kv_heads, head_dim)
    scores = jnp.einsum("qkgd,nkd->kgqn", query_heads, key_heads) * (head_dim ** -0.5)
    scores = jnp.where(allowed[None, None], scores, -1e30)
    block_max = jnp.max(scores, axis=-1)
    exp_terms = jnp.where(allowed[None, None], jnp.exp(scores - block_max[..., None]), 0.0)
    weight_sum = jnp.sum(exp_terms, axis=-1)
    prob_bf = lax.optimization_barrier(exp_terms.astype(jnp.bfloat16)).astype(jnp.float32)
    value_heads = values.astype(jnp.float32).reshape(key_count, kv_heads, head_dim)
    blended = jnp.einsum("kgqn,nkd->qkgd", prob_bf, value_heads)
    floor_sum = jnp.maximum(weight_sum, 1.0).transpose(2, 0, 1)[..., None]
    blended = (blended / floor_sum).reshape(row_count, full_width).astype(jnp.bfloat16)
    maxima = block_max.transpose(2, 0, 1).reshape(row_count, -1)
    weights = weight_sum.transpose(2, 0, 1).reshape(row_count, -1)
    return blended, maxima, weights


def combine(running, part, head_count):
    summed, maxima, weights = running
    blended, part_max, part_weight = part
    row_count, full_width = summed.shape
    highest = jnp.maximum(maxima, part_max)
    old_scale = jnp.exp(maxima - highest)
    new_scale = part_weight * jnp.exp(part_max - highest)
    summed = summed.reshape(row_count, head_count, -1) * old_scale[:, :, None]
    summed = summed + new_scale[:, :, None] * blended.astype(jnp.float32).reshape(row_count, head_count, -1)
    return summed.reshape(row_count, full_width), highest, weights * old_scale + new_scale


def one_request(items):
    query_rows, cache_k, cache_v, fresh_k, fresh_v, hit_limit, filled, block_order = items
    full_width = query_rows.shape[1]
    head_count = full_width // HEAD_DIM
    kv_heads = fresh_k.shape[1] // HEAD_DIM
    lanes = jnp.arange(NEW, dtype=jnp.int32)
    query_pos = block_order[lanes // Q_DEV] * Q_DEV + lanes % Q_DEV
    cache_lane = jnp.arange(C_DEV, dtype=jnp.int32)
    fresh_lane = jnp.arange(Q_DEV, dtype=jnp.int32)
    start = (jnp.zeros((NEW, full_width), jnp.float32), jnp.full((NEW, head_count), -1e30, jnp.float32), jnp.zeros((NEW, head_count), jnp.float32))

    def add_block(running, block_index):
        cache_first = (block_index * C_DEV).astype(jnp.int32)
        fresh_first = (block_index * Q_DEV).astype(jnp.int32)
        keys_here = jnp.concatenate([lax.dynamic_slice_in_dim(cache_k, cache_first, C_DEV, 0), lax.dynamic_slice_in_dim(fresh_k, fresh_first, Q_DEV, 0)], 0)
        values_here = jnp.concatenate([lax.dynamic_slice_in_dim(cache_v, cache_first, C_DEV, 0), lax.dynamic_slice_in_dim(fresh_v, fresh_first, Q_DEV, 0)], 0)
        cache_ok = (block_index * C_DEV + cache_lane) < hit_limit
        fresh_ok = (block_order[block_index] * Q_DEV + fresh_lane)[None, :] <= query_pos[:, None]
        allowed = jnp.concatenate([jnp.broadcast_to(cache_ok[None, :], (NEW, C_DEV)), fresh_ok], 1)
        part = partial_block(query_rows, keys_here, values_here, allowed, kv_heads)
        return combine(running, part, head_count), None

    running, _ = lax.scan(add_block, start, jnp.arange(N_BLK, dtype=jnp.int32))
    summed, maxima, weights = running
    blended = (summed.reshape(NEW, head_count, -1) / weights[:, :, None]).reshape(NEW, full_width)
    blended = jnp.where((query_pos < filled)[:, None], blended, 0.0)
    return blended.astype(jnp.bfloat16)


def reference(queries, cache_keys, cache_values, new_keys, new_values, hits, counts, assign):
    return lax.map(one_request, (queries, cache_keys, cache_values, new_keys, new_values, hits, counts, assign))
```

```python
import functools
import math

import jax
import jax.numpy as jnp
from jax import lax
from jax.experimental import pallas as pl
from jax.experimental.pallas import tpu as pltpu
from jax.sharding import PartitionSpec as P

HEAD_DIM = 128
FLOOR = -1e30
MESH = pl.DeviceIdType.MESH


def kernel(
    n_blk, n_grp, size, per_chunk,
    hits_ref, counts_ref, assign_ref, q_ref, nk_ref, nv_ref, ck_ref, cv_ref, out_ref,
    k_own, v_own, k_buf, v_buf, vt_buf, fresh_own, fresh_buf, q_buf, o_buf, r_buf,
    load_sem, kv_send, kv_recv, fresh_send, fresh_recv, q_send, q_recv, o_send, o_recv,
):
    blk, grp = lax.axis_index("blk"), lax.axis_index("grp")
    n_dev = n_blk * n_grp
    cluster, member = blk // size, blk % size
    n_cluster = n_blk // size
    requests, rows, heads, dim = q_ref.shape
    group = heads // size
    half = fresh_own.shape[2] // 2
    cached = k_own.shape[0]
    block_rows = rows * n_grp
    n_chunk = n_blk // per_chunk
    lanes = per_chunk * block_rows * group
    rate = dim ** -0.5 * math.log2(math.e)

    load_k = pltpu.make_async_copy(ck_ref.at[0], k_own, load_sem.at[0])
    load_v = pltpu.make_async_copy(cv_ref.at[0], v_own, load_sem.at[1])
    load_k.start()
    load_v.start()

    barrier = pltpu.get_barrier_semaphore()

    def peer(step):
        return lax.rem(blk + step // n_grp, n_blk), lax.rem(grp + step % n_grp, n_grp)

    def greet(step, carry):
        to_blk, to_grp = peer(step)
        pl.semaphore_signal(
            barrier, inc=1, device_id={"blk": to_blk, "grp": to_grp}, device_id_type=MESH
        )
        return carry

    lax.fori_loop(1, n_dev, greet, 0)

    fresh_own[...] = jnp.zeros_like(fresh_own)
    for r in range(requests):
        for h in range(size):
            cols = slice(h * dim, (h + 1) * dim)
            fresh_own[r, h, 0:rows, :] = nk_ref[r, :, cols].astype(jnp.float32)
            fresh_own[r, h, half : half + rows, :] = nv_ref[r, :, cols].astype(jnp.float32)

    pl.semaphore_wait(barrier, n_dev - 1)

    def q_piece(to_grp, head):
        return q_ref.at[to_grp, :, pl.ds(pl.multiple_of(head * group, group), group), :]

    def send_q(step, carry):
        to_blk, to_grp = peer(step)
        pltpu.make_async_remote_copy(
            src_ref=q_piece(to_grp, to_blk % size),
            dst_ref=q_buf.at[blk, grp],
            send_sem=q_send,
            recv_sem=q_recv.at[blk // per_chunk],
            device_id={"blk": to_blk, "grp": to_grp},
            device_id_type=MESH,
        ).start()
        return carry

    lax.fori_loop(1, n_dev, send_q, 0)
    pltpu.make_async_copy(
        q_piece(grp, member), q_buf.at[blk, grp], q_recv.at[blk // per_chunk]
    ).start()

    load_k.wait()
    load_v.wait()
    kv_copies = []
    for step in range(1, size):
        to_member = lax.rem(member + step, size)
        cols = pl.ds(pl.multiple_of(to_member * dim, dim), dim)
        for which, (own, buf) in enumerate(((k_own, k_buf), (v_own, v_buf))):
            copy = pltpu.make_async_remote_copy(
                src_ref=own.at[:, cols],
                dst_ref=buf.at[member],
                send_sem=kv_send.at[step, which],
                recv_sem=kv_recv.at[step, which],
                device_id={"blk": cluster * size + to_member, "grp": grp},
                device_id_type=MESH,
            )
            copy.start()
            kv_copies.append(copy)
    own_cols = pl.ds(pl.multiple_of(member * dim, dim), dim)
    for which, (own, buf) in enumerate(((k_own, k_buf), (v_own, v_buf))):
        copy = pltpu.make_async_copy(own.at[:, own_cols], buf.at[member], kv_recv.at[0, which])
        copy.start()
        kv_copies.append(copy)

    def send_fresh(step, carry):
        to_member = lax.rem(member + step // n_grp, size)
        to_grp = lax.rem(grp + step % n_grp, n_grp)
        pltpu.make_async_remote_copy(
            src_ref=fresh_own.at[to_grp, to_member],
            dst_ref=fresh_buf.at[member * n_grp + grp],
            send_sem=fresh_send,
            recv_sem=fresh_recv,
            device_id={"blk": cluster * size + to_member, "grp": to_grp},
            device_id_type=MESH,
        ).start()
        return carry

    lax.fori_loop(1, size * n_grp, send_fresh, 0)
    pltpu.make_async_copy(
        fresh_own.at[grp, member], fresh_buf.at[member * n_grp + grp], fresh_recv
    ).start()

    pltpu.make_async_copy(fresh_buf, fresh_buf, fresh_recv).wait()
    for copy in kv_copies:
        copy.wait()

    hit = hits_ref[0]
    count = counts_ref[0]
    n_fresh = size * n_grp * 2 * half
    fresh = fresh_buf[...].reshape(n_fresh, dim).astype(jnp.bfloat16)
    for s in range(size):
        vt_buf[:, s * cached : (s + 1) * cached] = v_buf[s].T
    vt_buf[:, size * cached :] = fresh.T

    key_row = lax.broadcasted_iota(jnp.int32, (n_fresh, 1), 0)
    key_from = key_row // (2 * half)
    key_pos = (key_from % n_grp) * rows + key_row % (2 * half)
    for s in range(size):
        base = assign_ref[0, cluster * size + s] * block_rows
        key_pos = key_pos + jnp.where(key_from // n_grp == s, base, 0)
    key_real = key_row % (2 * half) < rows
    key_pos = jnp.where(key_real, key_pos, n_blk * block_rows)
    first = cluster * size * cached
    cached_ok = first + lax.broadcasted_iota(jnp.int32, (size * cached, 1), 0) < hit

    def chunk_step(turn, carry):
        chunk = lax.rem(blk // per_chunk + turn + 1, n_chunk)
        blocks = pl.ds(chunk * per_chunk, per_chunk)
        pltpu.make_async_copy(q_buf.at[blocks], q_buf.at[blocks], q_recv.at[chunk]).wait()
        queries = q_buf[blocks].reshape(lanes, dim)
        lane = lax.broadcasted_iota(jnp.int32, (1, lanes), 1)
        pos = (lane // group) % block_rows
        for j in range(per_chunk):
            base = assign_ref[0, chunk * per_chunk + j] * block_rows
            pos = pos + jnp.where(lane // (group * block_rows) == j, base, 0)
        nt = (((1,), (1,)), ((), ()))
        keys = k_buf[...].reshape(size * cached, dim)
        s_old = lax.dot_general(keys, queries, nt, preferred_element_type=jnp.float32)
        s_new = lax.dot_general(fresh, queries, nt, preferred_element_type=jnp.float32)
        s_old = jnp.where(cached_ok, s_old, FLOOR)
        s_new = jnp.where(key_pos <= pos, s_new, FLOOR)
        top = jnp.maximum(
            jnp.max(s_old, axis=0, keepdims=True), jnp.max(s_new, axis=0, keepdims=True)
        )
        top = jnp.maximum(top, 0.1 * FLOOR)
        p_old = jnp.exp2((s_old - top) * rate)
        p_new = jnp.exp2((s_new - top) * rate)
        weight = jnp.sum(p_old, axis=0, keepdims=True) + jnp.sum(p_new, axis=0, keepdims=True)
        p_new = pltpu.roll(p_new, half, 0)
        nn = (((1,), (0,)), ((), ()))
        mixed = lax.dot_general(
            vt_buf[:, : size * cached], p_old.astype(jnp.bfloat16), nn,
            preferred_element_type=jnp.float32,
        ) + lax.dot_general(
            vt_buf[:, size * cached :], p_new.astype(jnp.bfloat16), nn,
            preferred_element_type=jnp.float32,
        )
        mixed = jnp.where(pos < count, mixed / jnp.maximum(weight, 1.0), 0.0)
        level = top * rate + jnp.log2(jnp.maximum(weight, 1e-30))
        n_dest = per_chunk * n_grp
        values = mixed.T.reshape(per_chunk, n_grp, rows, group, dim)
        levels = jnp.broadcast_to(level, (dim, lanes)).T.reshape(n_dest, rows, group, dim)
        spot = lax.broadcasted_iota(jnp.int32, (1, 1, dim), 2)
        tile = jnp.zeros((n_dest, group, dim), jnp.float32)
        for i in range(rows):
            tile = jnp.where(spot % rows == i, levels[:, i], tile)
        high = tile.astype(jnp.bfloat16).astype(jnp.float32)
        middle = (tile - high).astype(jnp.bfloat16).astype(jnp.float32)
        low = tile - high - middle
        tile = jnp.where(spot < rows, high, jnp.where(spot < 2 * rows, middle, low))
        tile = jnp.where(spot < 3 * rows, tile, 0.0)
        o_buf[blocks, :, 0:rows] = values.astype(jnp.bfloat16)
        o_buf[blocks, :, rows : rows + 1] = tile.astype(jnp.bfloat16).reshape(
            per_chunk, n_grp, 1, group, dim
        )

        def send_out(index, carry):
            to_blk = chunk * per_chunk + index // n_grp
            to_grp = index % n_grp
            mine = jnp.logical_and(to_blk == blk, to_grp == grp)

            @pl.when(mine)
            def _():
                pltpu.make_async_copy(o_buf.at[blk, grp], r_buf.at[blk, grp], o_recv).start()

            @pl.when(jnp.logical_not(mine))
            def _():
                pltpu.make_async_remote_copy(
                    src_ref=o_buf.at[to_blk, to_grp],
                    dst_ref=r_buf.at[blk, grp],
                    send_sem=o_send,
                    recv_sem=o_recv,
                    device_id={"blk": to_blk, "grp": to_grp},
                    device_id_type=MESH,
                ).start()

            return carry

        lax.fori_loop(0, n_dest, send_out, 0)
        return carry

    lax.fori_loop(0, n_chunk, chunk_step, 0)

    pltpu.make_async_copy(r_buf, r_buf, o_recv).wait()

    def parts(c, h, r):
        tile = r_buf[c * size + h, r, rows].astype(jnp.float32)
        return tile + pltpu.roll(tile, dim - rows, 1) + pltpu.roll(tile, dim - 2 * rows, 1)

    def finish(r, carry):
        for h in range(size):
            levels = [parts(c, h, r) for c in range(n_cluster)]
            top = functools.reduce(jnp.maximum, levels)
            scales = [jnp.exp2(level - top) for level in levels]
            total = functools.reduce(jnp.add, scales)
            scales = [scale / total for scale in scales]
            for i in range(rows):
                terms = [
                    scales[c][:, i : i + 1] * r_buf[c * size + h, r, i].astype(jnp.float32)
                    for c in range(n_cluster)
                ]
                out_ref[r, i, h * group : (h + 1) * group, :] = functools.reduce(
                    jnp.add, terms
                ).astype(out_ref.dtype)
        return carry

    lax.fori_loop(0, requests, finish, 0)

    rest = n_dev - 1
    q_flat = q_buf.at[0 : n_blk - 1]
    pltpu.make_async_copy(q_flat, q_flat, q_send).wait()
    q_flat = q_buf.at[0, 0 : n_grp - 1]
    pltpu.make_async_copy(q_flat, q_flat, q_send).wait()
    r_flat = r_buf.at[0 : n_blk - 1]
    pltpu.make_async_copy(r_flat, r_flat, o_send).wait()
    r_flat = r_buf.at[0, 0 : n_grp - 1]
    pltpu.make_async_copy(r_flat, r_flat, o_send).wait()
    f_flat = fresh_buf.at[0 : size * n_grp - 1]
    pltpu.make_async_copy(f_flat, f_flat, fresh_send).wait()


def solution(mesh):
    n_blk, n_grp = mesh.shape["blk"], mesh.shape["grp"]

    def local(queries, cache_keys, cache_values, new_keys, new_values, hits, counts, assign):
        requests, rows, width = queries.shape
        cached, kv_width = cache_keys.shape[1:]
        size = kv_width // HEAD_DIM
        heads = width // HEAD_DIM
        group = heads // size
        half = max(rows, 4)
        per_chunk = 2
        bf, f32 = jnp.bfloat16, jnp.float32
        vmem = pl.BlockSpec(memory_space=pltpu.VMEM)
        smem = pl.BlockSpec(memory_space=pltpu.SMEM)
        hbm = pl.BlockSpec(memory_space=pl.ANY)
        n_keys = size * cached + size * n_grp * 2 * half
        out = pl.pallas_call(
            functools.partial(kernel, n_blk, n_grp, size, per_chunk),
            out_shape=jax.ShapeDtypeStruct((requests, rows, heads, HEAD_DIM), bf),
            in_specs=[smem, smem, smem, vmem, vmem, vmem, hbm, hbm],
            out_specs=vmem,
            scratch_shapes=[
                pltpu.VMEM((cached, kv_width), bf),
                pltpu.VMEM((cached, kv_width), bf),
                pltpu.VMEM((size, cached, HEAD_DIM), bf),
                pltpu.VMEM((size, cached, HEAD_DIM), bf),
                pltpu.VMEM((HEAD_DIM, n_keys), bf),
                pltpu.VMEM((requests, size, 2 * half, HEAD_DIM), f32),
                pltpu.VMEM((size * n_grp, 2 * half, HEAD_DIM), f32),
                pltpu.VMEM((n_blk, n_grp, rows, group, HEAD_DIM), bf),
                pltpu.VMEM((n_blk, n_grp, rows + 1, group, HEAD_DIM), bf),
                pltpu.VMEM((n_blk, n_grp, rows + 1, group, HEAD_DIM), bf),
                pltpu.SemaphoreType.DMA((2,)),
                pltpu.SemaphoreType.DMA((size, 2)),
                pltpu.SemaphoreType.DMA((size, 2)),
                pltpu.SemaphoreType.DMA,
                pltpu.SemaphoreType.DMA,
                pltpu.SemaphoreType.DMA,
                pltpu.SemaphoreType.DMA((n_blk // per_chunk,)),
                pltpu.SemaphoreType.DMA,
                pltpu.SemaphoreType.DMA,
            ],
            compiler_params=pltpu.CompilerParams(
                collective_id=0, has_side_effects=True, vmem_limit_bytes=60 * 2**20
            ),
        )(
            hits, counts, assign,
            queries.reshape(requests, rows, heads, HEAD_DIM),
            new_keys, new_values, cache_keys, cache_values,
        )
        return out.reshape(requests, rows, width)

    return jax.shard_map(
        local,
        mesh=mesh,
        in_specs=(
            P(None, ("blk", "grp"), None),
            P("grp", "blk", None),
            P("grp", "blk", None),
            P(None, ("blk", "grp"), None),
            P(None, ("blk", "grp"), None),
            P("grp"),
            P("grp"),
            P("grp", None),
        ),
        out_specs=P(None, ("blk", "grp"), None),
        check_vma=False,
    )
```

```python
import functools
import math

import jax
import jax.numpy as jnp
from jax import lax
from jax.experimental import pallas as pl
from jax.experimental.pallas import tpu as pltpu
from jax.sharding import PartitionSpec as P

HEAD_DIM = 128
FLOOR = -1e30
MESH = pl.DeviceIdType.MESH


def kernel(
    n_blk, n_grp, size, per_chunk,
    hits_ref, counts_ref, assign_ref, q_ref, nk_ref, nv_ref, ck_ref, cv_ref, out_ref,
    q_own, k_own, v_own, k_buf, v_buf, vt_buf, fresh_own, fresh_buf, q_buf, o_buf, r_buf,
    known_sem, load_sem, kv_send, kv_recv, fresh_send, fresh_recv, q_send, q_recv, o_send, o_recv,
):
    blk, grp = lax.axis_index("blk"), lax.axis_index("grp")
    n_dev = n_blk * n_grp
    cluster, member = blk // size, blk % size
    n_cluster = n_blk // size
    requests, rows, heads, dim = q_own.shape
    group = heads // size
    half = fresh_own.shape[2] // 2
    cached = k_own.shape[0]
    block_rows = rows * n_grp
    n_chunk = n_blk // per_chunk
    lanes = per_chunk * block_rows * group
    rate = dim ** -0.5 * math.log2(math.e)

    load_k = pltpu.make_async_copy(ck_ref.at[0], k_own, load_sem.at[0])
    load_v = pltpu.make_async_copy(cv_ref.at[0], v_own, load_sem.at[1])
    load_k.start()
    load_v.start()

    barrier = pltpu.get_barrier_semaphore()

    def peer(step):
        return lax.rem(blk + step // n_grp, n_blk), lax.rem(grp + step % n_grp, n_grp)

    grp_peers = [(blk, lax.rem(grp + step, n_grp)) for step in range(1, n_grp)]
    cluster_peers = [
        (cluster * size + lax.rem(member + step, size), grp) for step in range(1, size)
    ]
    far_peers = [(lax.rem(blk + step * size, n_blk), grp) for step in range(1, n_cluster)]

    def meet(sem, peers):
        for to_blk, to_grp in peers:
            pl.semaphore_signal(
                sem, inc=1, device_id={"blk": to_blk, "grp": to_grp}, device_id_type=MESH
            )

    near = grp_peers + cluster_peers + far_peers
    meet(barrier, near)

    gap = jnp.zeros((half - rows, dim), jnp.float32)
    for r in range(requests):
        for h in range(size):
            cols = slice(h * dim, (h + 1) * dim)
            pieces = [nk_ref[r, :, cols].astype(jnp.float32), nv_ref[r, :, cols].astype(jnp.float32)]
            if half > rows:
                pieces = [pieces[0], gap, pieces[1], gap]
            fresh_own[r, h] = jnp.concatenate(pieces, 0).astype(jnp.bfloat16)
        q_own[r] = q_ref[r].reshape(rows, heads, dim)

    pl.semaphore_wait(barrier, len(near))

    load_k.wait()
    load_v.wait()
    kv_copies = []
    for step in range(1, size):
        to_member = lax.rem(member + step, size)
        cols = pl.ds(pl.multiple_of(to_member * dim, dim), dim)
        for which, (own, buf) in enumerate(((k_own, k_buf), (v_own, v_buf))):
            copy = pltpu.make_async_remote_copy(
                src_ref=own.at[:, cols],
                dst_ref=buf.at[member],
                send_sem=kv_send.at[step, which],
                recv_sem=kv_recv.at[step, which],
                device_id={"blk": cluster * size + to_member, "grp": grp},
                device_id_type=MESH,
            )
            copy.start()
            kv_copies.append(copy)
    own_cols = pl.ds(pl.multiple_of(member * dim, dim), dim)
    for which, (own, buf) in enumerate(((k_own, k_buf), (v_own, v_buf))):
        copy = pltpu.make_async_copy(own.at[:, own_cols], buf.at[member], kv_recv.at[0, which])
        copy.start()
        kv_copies.append(copy)

    meet(known_sem.at[0], grp_peers)
    pl.semaphore_wait(known_sem.at[0], len(grp_peers))
    meet(known_sem.at[1], cluster_peers)
    pl.semaphore_wait(known_sem.at[1], len(cluster_peers))

    def send_fresh(step, carry):
        to_member = lax.rem(member + step // n_grp, size)
        to_grp = lax.rem(grp + step % n_grp, n_grp)
        pltpu.make_async_remote_copy(
            src_ref=fresh_own.at[to_grp, to_member],
            dst_ref=fresh_buf.at[member * n_grp + grp],
            send_sem=fresh_send,
            recv_sem=fresh_recv,
            device_id={"blk": cluster * size + to_member, "grp": to_grp},
            device_id_type=MESH,
        ).start()
        return carry

    lax.fori_loop(1, size * n_grp, send_fresh, 0)
    pltpu.make_async_copy(
        fresh_own.at[grp, member], fresh_buf.at[member * n_grp + grp], fresh_recv
    ).start()

    def q_piece(to_grp, head):
        return q_own.at[to_grp, :, pl.ds(pl.multiple_of(head * group, group), group), :]

    def send_q(step, carry):
        to_blk, to_grp = peer(step)
        pltpu.make_async_remote_copy(
            src_ref=q_piece(to_grp, to_blk % size),
            dst_ref=q_buf.at[blk, grp],
            send_sem=q_send,
            recv_sem=q_recv.at[blk // per_chunk],
            device_id={"blk": to_blk, "grp": to_grp},
            device_id_type=MESH,
        ).start()
        return carry

    lax.fori_loop(1, n_dev, send_q, 0)
    pltpu.make_async_copy(
        q_piece(grp, member), q_buf.at[blk, grp], q_recv.at[blk // per_chunk]
    ).start()

    pltpu.make_async_copy(fresh_buf, fresh_buf, fresh_recv).wait()
    for copy in kv_copies:
        copy.wait()

    hit = hits_ref[0]
    count = counts_ref[0]
    n_fresh = size * n_grp * 2 * half
    fresh = fresh_buf[...].reshape(n_fresh, dim)
    for s in range(size):
        vt_buf[:, s * cached : (s + 1) * cached] = v_buf[s].T
    vt_buf[:, size * cached :] = fresh.T

    key_row = lax.broadcasted_iota(jnp.int32, (n_fresh, 1), 0)
    key_from = key_row // (2 * half)
    key_pos = (key_from % n_grp) * rows + key_row % (2 * half)
    for s in range(size):
        base = assign_ref[0, cluster * size + s] * block_rows
        key_pos = key_pos + jnp.where(key_from // n_grp == s, base, 0)
    key_real = key_row % (2 * half) < rows
    key_pos = jnp.where(key_real, key_pos, n_blk * block_rows)
    first = cluster * size * cached
    cached_ok = first + lax.broadcasted_iota(jnp.int32, (size * cached, 1), 0) < hit

    def chunk_step(turn, carry):
        chunk = lax.rem(blk // per_chunk + turn + 1, n_chunk)
        blocks = pl.ds(chunk * per_chunk, per_chunk)
        pltpu.make_async_copy(q_buf.at[blocks], q_buf.at[blocks], q_recv.at[chunk]).wait()
        queries = q_buf[blocks].reshape(lanes, dim)
        lane = lax.broadcasted_iota(jnp.int32, (1, lanes), 1)
        pos = (lane // group) % block_rows
        for j in range(per_chunk):
            base = assign_ref[0, chunk * per_chunk + j] * block_rows
            pos = pos + jnp.where(lane // (group * block_rows) == j, base, 0)
        nt = (((1,), (1,)), ((), ()))
        keys = k_buf[...].reshape(size * cached, dim)
        s_old = lax.dot_general(keys, queries, nt, preferred_element_type=jnp.float32)
        s_new = lax.dot_general(fresh, queries, nt, preferred_element_type=jnp.float32)
        s_old = jnp.where(cached_ok, s_old, FLOOR)
        s_new = jnp.where(key_pos <= pos, s_new, FLOOR)
        top = jnp.maximum(
            jnp.max(s_old, axis=0, keepdims=True), jnp.max(s_new, axis=0, keepdims=True)
        )
        top = jnp.maximum(top, 0.1 * FLOOR)
        p_old = jnp.exp2((s_old - top) * rate)
        p_new = jnp.exp2((s_new - top) * rate)
        weight = jnp.sum(p_old, axis=0, keepdims=True) + jnp.sum(p_new, axis=0, keepdims=True)
        p_new = pltpu.roll(p_new, half, 0)
        nn = (((1,), (0,)), ((), ()))
        mixed = lax.dot_general(
            vt_buf[:, : size * cached], p_old.astype(jnp.bfloat16), nn,
            preferred_element_type=jnp.float32,
        ) + lax.dot_general(
            vt_buf[:, size * cached :], p_new.astype(jnp.bfloat16), nn,
            preferred_element_type=jnp.float32,
        )
        mixed = jnp.where(pos < count, mixed / jnp.maximum(weight, 1.0), 0.0)
        level = top * rate + jnp.log2(jnp.maximum(weight, 1e-30))
        n_dest = per_chunk * n_grp
        values = mixed.T.reshape(per_chunk, n_grp, rows, group, dim)
        levels = jnp.broadcast_to(level, (dim, lanes)).T.reshape(n_dest, rows, group, dim)
        spot = lax.broadcasted_iota(jnp.int32, (1, 1, dim), 2)
        tile = jnp.zeros((n_dest, group, dim), jnp.float32)
        for i in range(rows):
            tile = jnp.where(spot % rows == i, levels[:, i], tile)
        high = tile.astype(jnp.bfloat16).astype(jnp.float32)
        middle = (tile - high).astype(jnp.bfloat16).astype(jnp.float32)
        low = tile - high - middle
        tile = jnp.where(spot < rows, high, jnp.where(spot < 2 * rows, middle, low))
        tile = jnp.where(spot < 3 * rows, tile, 0.0)
        o_buf[blocks, :, 0:rows] = values.astype(jnp.bfloat16)
        o_buf[blocks, :, rows : rows + 1] = tile.astype(jnp.bfloat16).reshape(
            per_chunk, n_grp, 1, group, dim
        )

        def send_out(index, carry):
            to_blk = chunk * per_chunk + index // n_grp
            to_grp = index % n_grp
            mine = jnp.logical_and(to_blk == blk, to_grp == grp)

            @pl.when(mine)
            def _():
                pltpu.make_async_copy(o_buf.at[blk, grp], r_buf.at[blk, grp], o_recv).start()

            @pl.when(jnp.logical_not(mine))
            def _():
                pltpu.make_async_remote_copy(
                    src_ref=o_buf.at[to_blk, to_grp],
                    dst_ref=r_buf.at[blk, grp],
                    send_sem=o_send,
                    recv_sem=o_recv,
                    device_id={"blk": to_blk, "grp": to_grp},
                    device_id_type=MESH,
                ).start()

            return carry

        lax.fori_loop(0, n_dest, send_out, 0)
        return carry

    lax.fori_loop(0, n_chunk, chunk_step, 0)

    pltpu.make_async_copy(r_buf, r_buf, o_recv).wait()

    def parts(c, h, r):
        tile = r_buf[c * size + h, r, rows].astype(jnp.float32)
        return tile + pltpu.roll(tile, dim - rows, 1) + pltpu.roll(tile, dim - 2 * rows, 1)

    def finish(r, carry):
        for h in range(size):
            levels = [parts(c, h, r) for c in range(n_cluster)]
            top = functools.reduce(jnp.maximum, levels)
            scales = [jnp.exp2(level - top) for level in levels]
            total = functools.reduce(jnp.add, scales)
            scales = [scale / total for scale in scales]
            for i in range(rows):
                terms = [
                    scales[c][:, i : i + 1] * r_buf[c * size + h, r, i].astype(jnp.float32)
                    for c in range(n_cluster)
                ]
                out_ref[r, i, h * group : (h + 1) * group, :] = functools.reduce(
                    jnp.add, terms
                ).astype(out_ref.dtype)
        return carry

    lax.fori_loop(0, requests, finish, 0)

    rest = n_dev - 1
    q_flat = q_buf.at[0 : n_blk - 1]
    pltpu.make_async_copy(q_flat, q_flat, q_send).wait()
    q_flat = q_buf.at[0, 0 : n_grp - 1]
    pltpu.make_async_copy(q_flat, q_flat, q_send).wait()
    r_flat = r_buf.at[0 : n_blk - 1]
    pltpu.make_async_copy(r_flat, r_flat, o_send).wait()
    r_flat = r_buf.at[0, 0 : n_grp - 1]
    pltpu.make_async_copy(r_flat, r_flat, o_send).wait()
    f_flat = fresh_buf.at[0 : size * n_grp - 1]
    pltpu.make_async_copy(f_flat, f_flat, fresh_send).wait()


def solution(mesh):
    n_blk, n_grp = mesh.shape["blk"], mesh.shape["grp"]

    def local(queries, cache_keys, cache_values, new_keys, new_values, hits, counts, assign):
        requests, rows, width = queries.shape
        cached, kv_width = cache_keys.shape[1:]
        size = kv_width // HEAD_DIM
        heads = width // HEAD_DIM
        group = heads // size
        half = max(rows, 4)
        per_chunk = 2
        bf, f32 = jnp.bfloat16, jnp.float32
        vmem = pl.BlockSpec(memory_space=pltpu.VMEM)
        smem = pl.BlockSpec(memory_space=pltpu.SMEM)
        hbm = pl.BlockSpec(memory_space=pl.ANY)
        n_keys = size * cached + size * n_grp * 2 * half
        out = pl.pallas_call(
            functools.partial(kernel, n_blk, n_grp, size, per_chunk),
            out_shape=jax.ShapeDtypeStruct((requests, rows, heads, HEAD_DIM), bf),
            in_specs=[smem, smem, smem, vmem, vmem, vmem, hbm, hbm],
            out_specs=vmem,
            scratch_shapes=[
                pltpu.VMEM((requests, rows, heads, HEAD_DIM), bf),
                pltpu.VMEM((cached, kv_width), bf),
                pltpu.VMEM((cached, kv_width), bf),
                pltpu.VMEM((size, cached, HEAD_DIM), bf),
                pltpu.VMEM((size, cached, HEAD_DIM), bf),
                pltpu.VMEM((HEAD_DIM, n_keys), bf),
                pltpu.VMEM((requests, size, 2 * half, HEAD_DIM), bf),
                pltpu.VMEM((size * n_grp, 2 * half, HEAD_DIM), bf),
                pltpu.VMEM((n_blk, n_grp, rows, group, HEAD_DIM), bf),
                pltpu.VMEM((n_blk, n_grp, rows + 1, group, HEAD_DIM), bf),
                pltpu.VMEM((n_blk, n_grp, rows + 1, group, HEAD_DIM), bf),
                pltpu.SemaphoreType.REGULAR((2,)),
                pltpu.SemaphoreType.DMA((2,)),
                pltpu.SemaphoreType.DMA((size, 2)),
                pltpu.SemaphoreType.DMA((size, 2)),
                pltpu.SemaphoreType.DMA,
                pltpu.SemaphoreType.DMA,
                pltpu.SemaphoreType.DMA,
                pltpu.SemaphoreType.DMA((n_blk // per_chunk,)),
                pltpu.SemaphoreType.DMA,
                pltpu.SemaphoreType.DMA,
            ],
            compiler_params=pltpu.CompilerParams(
                collective_id=0, has_side_effects=True, vmem_limit_bytes=60 * 2**20
            ),
        )(
            hits, counts, assign,
            queries, new_keys, new_values, cache_keys, cache_values,
        )
        return out.reshape(requests, rows, width)

    return jax.shard_map(
        local,
        mesh=mesh,
        in_specs=(
            P(None, ("blk", "grp"), None),
            P("grp", "blk", None),
            P("grp", "blk", None),
            P(None, ("blk", "grp"), None),
            P(None, ("blk", "grp"), None),
            P("grp"),
            P("grp"),
            P("grp", None),
        ),
        out_specs=P(None, ("blk", "grp"), None),
        check_vma=False,
    )
```

```python
import functools
import math

import jax
import jax.numpy as jnp
from jax import lax
from jax.experimental import pallas as pl
from jax.experimental.pallas import tpu as pltpu
from jax.sharding import PartitionSpec as P

HEAD_DIM = 128
FLOOR = -1e30
MESH = pl.DeviceIdType.MESH


def kernel(
    n_blk, n_grp, size, per_chunk,
    hits_ref, counts_ref, assign_ref, q_hbm, nk_hbm, nv_hbm, ck_ref, cv_ref, out_ref,
    q_ref, nk_ref, nv_ref, q_own, k_own, v_own, k_buf, v_buf, vt_buf, fresh_own, fresh_buf, q_buf, o_buf, r_buf, p_buf, w_buf, l_own, l_buf, scale_buf,
    known_sem, load_sem, kv_send, kv_recv, fresh_send, fresh_recv, q_send, q_recv, o_send, o_recv, l_send, l_recv,
):
    blk, grp = lax.axis_index("blk"), lax.axis_index("grp")
    n_dev = n_blk * n_grp
    cluster, member = blk // size, blk % size
    n_cluster = n_blk // size
    requests, rows, heads, dim = q_own.shape
    group = heads // size
    half = fresh_own.shape[2] // 2
    cached = k_own.shape[0]
    block_rows = rows * n_grp
    n_chunk = n_blk // per_chunk
    span = block_rows * group
    lanes = per_chunk * span
    rate = dim ** -0.5 * math.log2(math.e)

    barrier = pltpu.get_barrier_semaphore()

    def peer(step):
        return lax.rem(blk + step // n_grp, n_blk), lax.rem(grp + step % n_grp, n_grp)

    grp_peers = [(blk, lax.rem(grp + step, n_grp)) for step in range(1, n_grp)]
    cluster_peers = [
        (cluster * size + lax.rem(member + step, size), grp) for step in range(1, size)
    ]
    far_peers = [(lax.rem(blk + step * size, n_blk), grp) for step in range(1, n_cluster)]

    def meet(sem, peers):
        for to_blk, to_grp in peers:
            pl.semaphore_signal(
                sem, inc=1, device_id={"blk": to_blk, "grp": to_grp}, device_id_type=MESH
            )

    near = grp_peers + cluster_peers + far_peers
    meet(barrier, near)

    load_k = pltpu.make_async_copy(ck_ref.at[0], k_own, load_sem.at[0])
    load_v = pltpu.make_async_copy(cv_ref.at[0], v_own, load_sem.at[1])
    small = [
        pltpu.make_async_copy(source, target, load_sem.at[2 + i])
        for i, (source, target) in enumerate(
            ((q_hbm, q_ref), (nk_hbm, nk_ref), (nv_hbm, nv_ref))
        )
    ]
    load_k.start()
    load_v.start()
    for copy in small:
        copy.start()
    for copy in small:
        copy.wait()

    gap = jnp.zeros((half - rows, dim), jnp.float32)
    for r in range(requests):
        for h in range(size):
            cols = slice(h * dim, (h + 1) * dim)
            pieces = [nk_ref[r, :, cols].astype(jnp.float32), nv_ref[r, :, cols].astype(jnp.float32)]
            if half > rows:
                pieces = [pieces[0], gap, pieces[1], gap]
            fresh_own[r, h] = jnp.concatenate(pieces, 0).astype(jnp.bfloat16)
        q_own[r] = q_ref[r].reshape(rows, heads, dim)

    pl.semaphore_wait(barrier, len(near))

    own_cols = pl.ds(pl.multiple_of(member * dim, dim), dim)

    def send_heads(which, own, buf):
        copies = []
        for step in range(1, size):
            to_member = lax.rem(member + step, size)
            cols = pl.ds(pl.multiple_of(to_member * dim, dim), dim)
            copies.append(
                pltpu.make_async_remote_copy(
                    src_ref=own.at[:, cols],
                    dst_ref=buf.at[member],
                    send_sem=kv_send.at[step, which],
                    recv_sem=kv_recv.at[step, which],
                    device_id={"blk": cluster * size + to_member, "grp": grp},
                    device_id_type=MESH,
                )
            )
        copies.append(
            pltpu.make_async_copy(own.at[:, own_cols], buf.at[member], kv_recv.at[0, which])
        )
        for copy in copies:
            copy.start()
        return copies

    load_k.wait()
    k_copies = send_heads(0, k_own, k_buf)

    meet(known_sem.at[0], grp_peers)
    pl.semaphore_wait(known_sem.at[0], len(grp_peers))
    meet(known_sem.at[1], cluster_peers)
    pl.semaphore_wait(known_sem.at[1], len(cluster_peers))

    def send_fresh(step, carry):
        to_member = lax.rem(member + step // n_grp, size)
        to_grp = lax.rem(grp + step % n_grp, n_grp)
        pltpu.make_async_remote_copy(
            src_ref=fresh_own.at[to_grp, to_member],
            dst_ref=fresh_buf.at[member * n_grp + grp],
            send_sem=fresh_send,
            recv_sem=fresh_recv,
            device_id={"blk": cluster * size + to_member, "grp": to_grp},
            device_id_type=MESH,
        ).start()
        return carry

    lax.fori_loop(1, size * n_grp, send_fresh, 0)
    pltpu.make_async_copy(
        fresh_own.at[grp, member], fresh_buf.at[member * n_grp + grp], fresh_recv
    ).start()

    def q_piece(to_grp, head):
        return q_own.at[to_grp, :, pl.ds(pl.multiple_of(head * group, group), group), :]

    def send_q(step, carry):
        to_blk, to_grp = peer(n_dev - step)
        pltpu.make_async_remote_copy(
            src_ref=q_piece(to_grp, to_blk % size),
            dst_ref=q_buf.at[blk, grp],
            send_sem=q_send,
            recv_sem=q_recv.at[blk // per_chunk],
            device_id={"blk": to_blk, "grp": to_grp},
            device_id_type=MESH,
        ).start()
        return carry

    lax.fori_loop(1, n_dev, send_q, 0)
    pltpu.make_async_copy(
        q_piece(grp, member), q_buf.at[blk, grp], q_recv.at[blk // per_chunk]
    ).start()

    load_v.wait()
    v_copies = send_heads(1, v_own, v_buf)

    pltpu.make_async_copy(fresh_buf, fresh_buf, fresh_recv).wait()
    for copy in k_copies:
        copy.wait()

    hit = hits_ref[0]
    count = counts_ref[0]
    n_fresh = size * n_grp * 2 * half
    fresh = fresh_buf[...].reshape(n_fresh, dim)
    vt_buf[:, size * cached :] = fresh.T

    key_row = lax.broadcasted_iota(jnp.int32, (n_fresh, 1), 0)
    key_from = key_row // (2 * half)
    key_pos = (key_from % n_grp) * rows + key_row % (2 * half)
    for s in range(size):
        base = assign_ref[0, cluster * size + s] * block_rows
        key_pos = key_pos + jnp.where(key_from // n_grp == s, base, 0)
    key_real = key_row % (2 * half) < rows
    key_pos = jnp.where(key_real, key_pos, n_blk * block_rows)
    first = cluster * size * cached
    cached_ok = first + lax.broadcasted_iota(jnp.int32, (size * cached, 1), 0) < hit

    def score_chunk(turn, carry):
        chunk = lax.rem(blk // per_chunk + turn + 1, n_chunk)
        blocks = pl.ds(chunk * per_chunk, per_chunk)
        pltpu.make_async_copy(q_buf.at[blocks], q_buf.at[blocks], q_recv.at[chunk]).wait()
        queries = q_buf[blocks].reshape(lanes, dim)
        lane = lax.broadcasted_iota(jnp.int32, (1, lanes), 1)
        pos = (lane // group) % block_rows
        for j in range(per_chunk):
            base = assign_ref[0, chunk * per_chunk + j] * block_rows
            pos = pos + jnp.where(lane // (group * block_rows) == j, base, 0)
        nt = (((1,), (1,)), ((), ()))
        keys = k_buf[...].reshape(size * cached, dim)
        s_old = lax.dot_general(keys, queries, nt, preferred_element_type=jnp.float32)
        s_new = lax.dot_general(fresh, queries, nt, preferred_element_type=jnp.float32)
        s_old = jnp.where(cached_ok, s_old, FLOOR)
        s_new = jnp.where(key_pos <= pos, s_new, FLOOR)
        top = jnp.maximum(
            jnp.max(s_old, axis=0, keepdims=True), jnp.max(s_new, axis=0, keepdims=True)
        )
        top = jnp.maximum(top, 0.1 * FLOOR)
        p_old = jnp.exp2((s_old - top) * rate)
        p_new = jnp.exp2((s_new - top) * rate)
        weight = jnp.sum(p_old, axis=0, keepdims=True) + jnp.sum(p_new, axis=0, keepdims=True)
        p_new = pltpu.roll(p_new, half, 0)
        p_buf[chunk, : size * cached] = p_old.astype(jnp.bfloat16)
        p_buf[chunk, size * cached :] = p_new.astype(jnp.bfloat16)
        w_buf[chunk] = jnp.where(pos < count, 1.0 / jnp.maximum(weight, 1.0), 0.0)
        level = top * rate + jnp.log2(jnp.maximum(weight, 1e-30))
        for j in range(per_chunk):
            l_own[chunk * per_chunk + j] = level[:, j * span : (j + 1) * span]
        return carry

    lax.fori_loop(0, n_chunk, score_chunk, 0)

    for copy in v_copies:
        copy.wait()
    for s in range(size):
        vt_buf[:, s * cached : (s + 1) * cached] = v_buf[s].T

    def value_chunk(turn, carry):
        chunk = lax.rem(blk // per_chunk + turn + 1, n_chunk)
        blocks = pl.ds(chunk * per_chunk, per_chunk)
        mixed = jnp.dot(vt_buf[...], p_buf[chunk], preferred_element_type=jnp.float32)
        mixed = mixed * w_buf[chunk]
        n_dest = per_chunk * n_grp
        values = mixed.T.reshape(per_chunk, n_grp, rows, group, dim)
        o_buf[blocks] = values.astype(jnp.bfloat16)

        def send_out(index, carry):
            to_blk = chunk * per_chunk + index // n_grp
            to_grp = index % n_grp
            mine = jnp.logical_and(to_blk == blk, to_grp == grp)

            @pl.when(mine)
            def _():
                pltpu.make_async_copy(o_buf.at[blk, grp], r_buf.at[blk, grp], o_recv).start()
                pltpu.make_async_copy(l_own.at[blk], l_buf.at[blk, grp], l_recv).start()

            @pl.when(jnp.logical_not(mine))
            def _():
                pltpu.make_async_remote_copy(
                    src_ref=o_buf.at[to_blk, to_grp],
                    dst_ref=r_buf.at[blk, grp],
                    send_sem=o_send,
                    recv_sem=o_recv,
                    device_id={"blk": to_blk, "grp": to_grp},
                    device_id_type=MESH,
                ).start()
                pltpu.make_async_remote_copy(
                    src_ref=l_own.at[to_blk],
                    dst_ref=l_buf.at[blk, grp],
                    send_sem=l_send,
                    recv_sem=l_recv,
                    device_id={"blk": to_blk, "grp": to_grp},
                    device_id_type=MESH,
                ).start()

            return carry

        lax.fori_loop(0, n_dest, send_out, 0)
        return carry

    lax.fori_loop(0, n_chunk, value_chunk, 0)

    pltpu.make_async_copy(l_buf, l_buf, l_recv).wait()
    levels = l_buf[...].reshape(n_cluster, size * n_grp, span)
    scales = jnp.exp2(levels - jnp.max(levels, axis=0, keepdims=True))
    scales = scales / jnp.sum(scales, axis=0, keepdims=True)
    mine = pl.ds(pl.multiple_of(grp * rows * group, rows * group), rows * group)
    shares = []
    for c in range(n_cluster):
        scale_buf[c] = scales[c].T
        shares.append(scale_buf[c, mine, :])
    pltpu.make_async_copy(r_buf, r_buf, o_recv).wait()
    for r in range(requests):
        for h in range(size):
            column = slice(h * n_grp + r, h * n_grp + r + 1)
            terms = [
                shares[c][:, column].reshape(rows, group, 1)
                * r_buf[c * size + h, r].astype(jnp.float32)
                for c in range(n_cluster)
            ]
            joined = functools.reduce(jnp.add, terms).reshape(rows, group * dim)
            cols = slice(h * group * dim, (h + 1) * group * dim)
            out_ref[r, :, cols] = joined.astype(out_ref.dtype)

    q_flat = q_buf.at[0 : n_blk - 1]
    pltpu.make_async_copy(q_flat, q_flat, q_send).wait()
    q_flat = q_buf.at[0, 0 : n_grp - 1]
    pltpu.make_async_copy(q_flat, q_flat, q_send).wait()
    r_flat = r_buf.at[0 : n_blk - 1]
    pltpu.make_async_copy(r_flat, r_flat, o_send).wait()
    r_flat = r_buf.at[0, 0 : n_grp - 1]
    pltpu.make_async_copy(r_flat, r_flat, o_send).wait()
    l_flat = l_buf.at[0 : n_blk - 1]
    pltpu.make_async_copy(l_flat, l_flat, l_send).wait()
    l_flat = l_buf.at[0, 0 : n_grp - 1]
    pltpu.make_async_copy(l_flat, l_flat, l_send).wait()
    f_flat = fresh_buf.at[0 : size * n_grp - 1]
    pltpu.make_async_copy(f_flat, f_flat, fresh_send).wait()


def solution(mesh):
    n_blk, n_grp = mesh.shape["blk"], mesh.shape["grp"]

    def local(queries, cache_keys, cache_values, new_keys, new_values, hits, counts, assign):
        requests, rows, width = queries.shape
        cached, kv_width = cache_keys.shape[1:]
        size = kv_width // HEAD_DIM
        heads = width // HEAD_DIM
        group = heads // size
        half = max(rows, 4)
        per_chunk = 2
        span = rows * n_grp * group
        bf, f32 = jnp.bfloat16, jnp.float32
        vmem = pl.BlockSpec(memory_space=pltpu.VMEM)
        smem = pl.BlockSpec(memory_space=pltpu.SMEM)
        hbm = pl.BlockSpec(memory_space=pl.ANY)
        n_keys = size * cached + size * n_grp * 2 * half
        out = pl.pallas_call(
            functools.partial(kernel, n_blk, n_grp, size, per_chunk),
            out_shape=jax.ShapeDtypeStruct((requests, rows, width), bf),
            in_specs=[smem, smem, smem, hbm, hbm, hbm, hbm, hbm],
            out_specs=vmem,
            scratch_shapes=[
                pltpu.VMEM(queries.shape, bf),
                pltpu.VMEM(new_keys.shape, bf),
                pltpu.VMEM(new_values.shape, bf),
                pltpu.VMEM((requests, rows, heads, HEAD_DIM), bf),
                pltpu.VMEM((cached, kv_width), bf),
                pltpu.VMEM((cached, kv_width), bf),
                pltpu.VMEM((size, cached, HEAD_DIM), bf),
                pltpu.VMEM((size, cached, HEAD_DIM), bf),
                pltpu.VMEM((HEAD_DIM, n_keys), bf),
                pltpu.VMEM((requests, size, 2 * half, HEAD_DIM), bf),
                pltpu.VMEM((size * n_grp, 2 * half, HEAD_DIM), bf),
                pltpu.VMEM((n_blk, n_grp, rows, group, HEAD_DIM), bf),
                pltpu.VMEM((n_blk, n_grp, rows, group, HEAD_DIM), bf),
                pltpu.VMEM((n_blk, n_grp, rows, group, HEAD_DIM), bf),
                pltpu.VMEM((n_blk // per_chunk, n_keys, per_chunk * span), bf),
                pltpu.VMEM((n_blk // per_chunk, 1, per_chunk * span), f32),
                pltpu.VMEM((n_blk, 1, span), f32),
                pltpu.VMEM((n_blk, n_grp, 1, span), f32),
                pltpu.VMEM((n_blk // size, span, size * n_grp), f32),
                pltpu.SemaphoreType.REGULAR((2,)),
                pltpu.SemaphoreType.DMA((5,)),
                pltpu.SemaphoreType.DMA((size, 2)),
                pltpu.SemaphoreType.DMA((size, 2)),
                pltpu.SemaphoreType.DMA,
                pltpu.SemaphoreType.DMA,
                pltpu.SemaphoreType.DMA,
                pltpu.SemaphoreType.DMA((n_blk // per_chunk,)),
                pltpu.SemaphoreType.DMA,
                pltpu.SemaphoreType.DMA,
                pltpu.SemaphoreType.DMA,
                pltpu.SemaphoreType.DMA,
            ],
            compiler_params=pltpu.CompilerParams(
                collective_id=0, has_side_effects=True, vmem_limit_bytes=60 * 2**20
            ),
        )(
            hits, counts, assign,
            queries, new_keys, new_values, cache_keys, cache_values,
        )
        return out

    return jax.shard_map(
        local,
        mesh=mesh,
        in_specs=(
            P(None, ("blk", "grp"), None),
            P("grp", "blk", None),
            P("grp", "blk", None),
            P(None, ("blk", "grp"), None),
            P(None, ("blk", "grp"), None),
            P("grp"),
            P("grp"),
            P("grp", None),
        ),
        out_specs=P(None, ("blk", "grp"), None),
        check_vma=False,
    )
```
